1024 devices in a mesh: row: 64 (over z, x), col: 16 (over y, core).
Axes of the slice: x: 4, y: 8, z: 16, core: 2. Of those that a mesh axis runs over, the one named last changes fastest.
Arguments:
- initial_heat: bfloat16 [48, 2048, 4096], P(None, 'row', 'col'), may hold values from -6 to 6
- layer_conductance: bfloat16 [47, 2048, 4096], P(None, 'row', 'col'), may hold values from 0.049804688 to 20
- layer_spacing: float32 [48], replicated, may hold values from 0.5 to 2
- submerged_layers: int32 [2048, 4096], P('row', 'col'), may hold values from 1 to 48
- water_indicator: int32 [2048, 4096], P('row', 'col'), may hold values from 0 to 1, as said below
- seafloor_distance: float32 [2048, 4096], P('row', 'col'), may hold values from 0.5 to 2
Outputs:
- diffused_heat: float32 [48, 2048, 4096], P(None, 'row', 'col')
- height: float32 [2048, 4096], P('row', 'col')
The draws below stay inside these ranges and needn't reach their ends.
Inputs may be any that keep to these rules, and one draw needn't show every extreme that they name: `water_indicator`: land lies in a few large regions and in scattered single cells.
All inputs are finite; a program needn't handle non-finite values.
Results may differ from the reference program's by a relative error of at most 0.0003.
Values sent between devices are 32-bit elements; how exact they have to be, the bound alone decides.
No kernel may reach another device: no remote copies, remote signals or barrier semaphores. Data moves between devices by JAX's collectives and lax.ppermute only.
A program may use at most 32 MiB of HBM per device.

```python
import math
import jax
import jax.numpy as jnp
from jax import lax

DEPTH_LAYERS = 48
PATCH_NORTH_SOUTH = 32
ITERS = 4
MESH_NORTH_SOUTH = 2048
MESH_EAST_WEST = 4096
N_ROW = 64


def draw_water_indicator(key, part):
    region_count = 6
    keys = jax.random.split(jax.random.fold_in(key, 7331), 5)
    lat_start = jax.random.randint(keys[0], (region_count,), 0, MESH_NORTH_SOUTH)
    lon_start = jax.random.randint(keys[1], (region_count,), 0, MESH_EAST_WEST)
    lat_span = jax.random.randint(keys[2], (region_count,), MESH_NORTH_SOUTH // 16 + 1, MESH_NORTH_SOUTH // 4 + 2)
    lon_span = jax.random.randint(keys[3], (region_count,), MESH_EAST_WEST // 16 + 1, MESH_EAST_WEST // 4 + 2)
    lat_index = jnp.arange(MESH_NORTH_SOUTH, dtype=jnp.int32)
    lon_index = jnp.arange(MESH_EAST_WEST, dtype=jnp.int32)
    inside_lat = (lat_index[None, :] >= lat_start[:, None]) & (lat_index[None, :] < lat_start[:, None] + lat_span[:, None])
    lon_offset = (lon_index[None, :] - lon_start[:, None]) % MESH_EAST_WEST
    inside_lon = lon_offset < lon_span[:, None]
    land = jnp.any(inside_lat[:, :, None] & inside_lon[:, None, :], axis=0)
    scattered = jax.random.randint(keys[4], (MESH_NORTH_SOUTH, MESH_EAST_WEST), 0, 10) == 0
    return jnp.where(land | scattered, 0, 1).astype(jnp.int32)


def set_ends(values, own_key, least, high):
    extent = values.shape
    place = [jax.random.randint(jax.random.fold_in(own_key, axis), (), 0, extent[axis]) for axis in range(len(extent))]
    values = values.at[tuple(place)].set(least)
    longest = extent.index(max(extent))
    place[longest] = (place[longest] + 1) % extent[longest]
    return values.at[tuple(place)].set(high)


def level_of(own_key, extent, shards, low, largest):
    def one(position, blocks):
        steps = jax.random.uniform(jax.random.fold_in(jax.random.fold_in(own_key, 6), position), (blocks,), jnp.float32, low / len(shards), largest / len(shards))
        return jnp.repeat(jnp.exp(steps), extent[position] // blocks).reshape((-1,) + (1,) * (len(extent) - position - 1))

    factor_of = one(*shards[0])
    for cut in shards[1:]:
        factor_of = factor_of * one(*cut)
    return factor_of


def normal_values(key, extent, deviation, most, pieces=(), kind=jnp.bfloat16):
    gain = level_of(key, extent, pieces, -0.22, 0.18) if pieces else 1.0
    array = jax.random.normal(key, extent, jnp.float32) * deviation * gain
    return jnp.minimum(jnp.maximum(array, -most), most).astype(kind)


def setup_inputs(seed: int = 0) -> dict:
    key_of = jax.random.split(jax.random.key(seed), 7)
    initial_heat = normal_values(key_of[0], (DEPTH_LAYERS, MESH_NORTH_SOUTH, MESH_EAST_WEST), 1.0, 6.0, ((1, 64), (2, 16)))
    layer_conductance = jnp.clip(jnp.exp(math.log(20.0) - 5.9953784 * jax.random.uniform(key_of[1], (DEPTH_LAYERS - 1, MESH_NORTH_SOUTH, MESH_EAST_WEST), jnp.float32) ** level_of(key_of[1], (DEPTH_LAYERS - 1, MESH_NORTH_SOUTH, MESH_EAST_WEST), ((1, 64), (2, 16)), -0.2, 0.2)), 0.049804688, 20.0).astype(jnp.bfloat16)
    layer_spacing = jnp.clip(jnp.exp(jax.random.uniform(key_of[2], (DEPTH_LAYERS,), jnp.float32, math.log(0.5), math.log(2.0))), 0.5, 2.0)
    submerged_layers = set_ends(jax.random.randint(key_of[3], (MESH_NORTH_SOUTH, MESH_EAST_WEST), 1, DEPTH_LAYERS + 1), jax.random.fold_in(key_of[3], 1), 1, DEPTH_LAYERS).astype(jnp.int32)
    water_indicator = draw_water_indicator(jax.random.fold_in(key_of[6], 71), 0)
    seafloor_distance = jnp.clip(jnp.exp(math.log(2.0) - 1.3862944 * jax.random.uniform(key_of[5], (MESH_NORTH_SOUTH, MESH_EAST_WEST), jnp.float32) ** level_of(key_of[5], (MESH_NORTH_SOUTH, MESH_EAST_WEST), ((0, 64), (1, 16)), -0.2, 0.2)), 0.5, 2.0)
    return {"initial_heat": initial_heat, "layer_conductance": layer_conductance, "layer_spacing": layer_spacing, "submerged_layers": submerged_layers, "water_indicator": water_indicator, "seafloor_distance": seafloor_distance}


surface_term = 0.5
compass = ((-1, -1, 0.5), (-1, 0, 1.0), (-1, 1, 0.5), (0, -1, 1.0), (0, 1, 1.0), (1, -1, 0.5), (1, 0, 1.0), (1, 1, 0.5))

def backward_euler_vertical_diffuse(initial_heat, layer_conductance, layer_spacing, submerged_layers):
    layer_pile = initial_heat.shape[0]
    index = jnp.arange(layer_pile - 1, dtype=jnp.int32)
    couple = layer_conductance.astype(jnp.float32) * (index[:, None, None] + 1 < submerged_layers[None]).astype(jnp.float32)
    zero_level = jnp.zeros((1,) + submerged_layers.shape, jnp.float32)
    below = jnp.concatenate([zero_level, couple], axis=0)
    above = jnp.concatenate([couple, zero_level], axis=0)
    spacing_profile = layer_spacing[:, None, None]
    driving_term = spacing_profile * initial_heat.astype(jnp.float32)
    centre = spacing_profile + below + above

    def forward(carry, level):
        ratio_prev, value_prev = carry
        lower_level, upper_level, centre_level, source_level = level
        pivot = centre_level - lower_level * ratio_prev
        ratio = upper_level / pivot
        value = (source_level + lower_level * value_prev) / pivot
        return ((ratio, value), (ratio, value))
    start = (jnp.zeros(submerged_layers.shape, jnp.float32), jnp.zeros(submerged_layers.shape, jnp.float32))
    unused, (ratios, values) = lax.scan(forward, start, (below, above, centre, driving_term))

    def backward(carry, level):
        ratio, value = level
        result = value + ratio * carry
        return (result, result)
    unused, diffused_heat = lax.scan(backward, jnp.zeros(submerged_layers.shape, jnp.float32), (ratios, values), reverse=True)
    return diffused_heat

def depth_forcing(diffused_heat, layer_spacing, submerged_layers, water_indicator):
    layer_pile = diffused_heat.shape[0]
    index = jnp.arange(layer_pile, dtype=jnp.int32)
    live = (index[:, None, None] < submerged_layers[None]).astype(jnp.float32)
    total = lax.optimization_barrier(jnp.sum(layer_spacing[:, None, None] * live * diffused_heat, axis=0))
    return water_indicator.astype(jnp.float32) * total / math.sqrt(layer_pile)

def neighbour(field, offset_row, offset_col, first, count):
    return jnp.roll(field[first + offset_row:first + offset_row + count], -offset_col, axis=1)

def couplings(height_field, ocean_field, first, count):
    here_height = height_field[first:first + count]
    here_ocean = ocean_field[first:first + count]
    weights = []
    for offset_row, offset_col, factor in compass:
        other_height = neighbour(height_field, offset_row, offset_col, first, count)
        other_ocean = neighbour(ocean_field, offset_row, offset_col, first, count)
        weights.append(factor * here_ocean * other_ocean * (0.5 * (here_height + other_height)))
    weights = jnp.stack(weights)
    return (weights, surface_term + lax.optimization_barrier(jnp.sum(weights, axis=0)))

def operate(field, weights, centre, first, count):
    result = centre * field[first:first + count]
    for slot, (offset_row, offset_col, factor) in enumerate(compass):
        result = result - weights[slot] * neighbour(field, offset_row, offset_col, first, count)
    return result

def chebyshev_scalars(top):
    theta = 0.5 * (top + surface_term)
    delta = 0.5 * (top - surface_term)
    return (theta, delta, theta / delta)

def reference(initial_heat, layer_conductance, layer_spacing, submerged_layers, water_indicator, seafloor_distance):

    def each_patch(block):
        temp_block, diff_block, wet_block, mask_block = block
        mixed_block = backward_euler_vertical_diffuse(temp_block, diff_block, layer_spacing, wet_block)
        return (mixed_block, depth_forcing(mixed_block, layer_spacing, wet_block, mask_block))
    heat_patches = jnp.moveaxis(initial_heat.reshape(DEPTH_LAYERS, N_ROW, PATCH_NORTH_SOUTH, MESH_EAST_WEST), 1, 0)
    diffusion_patches = jnp.moveaxis(layer_conductance.reshape(DEPTH_LAYERS - 1, N_ROW, PATCH_NORTH_SOUTH, MESH_EAST_WEST), 1, 0)
    diffused_patches, driving_patches = lax.map(each_patch, (heat_patches, diffusion_patches, submerged_layers.reshape(N_ROW, PATCH_NORTH_SOUTH, MESH_EAST_WEST), water_indicator.reshape(N_ROW, PATCH_NORTH_SOUTH, MESH_EAST_WEST)))
    diffused_heat = jnp.moveaxis(diffused_patches, 0, 1).reshape(DEPTH_LAYERS, MESH_NORTH_SOUTH, MESH_EAST_WEST)
    forcing = driving_patches.reshape(MESH_NORTH_SOUTH, MESH_EAST_WEST)
    height_pad = jnp.pad(seafloor_distance, ((1, 1), (0, 0)))
    ocean_pad = jnp.pad(water_indicator.astype(jnp.float32), ((1, 1), (0, 0)))
    weights, centre = couplings(height_pad, ocean_pad, 1, MESH_NORTH_SOUTH)
    top = jnp.max(2.0 * centre - surface_term)
    theta, delta, sigma = chebyshev_scalars(top)
    solution = jnp.zeros_like(forcing)
    residual = forcing
    direction = forcing / theta
    recur = 1.0 / sigma
    for step in range(ITERS):
        solution = solution + direction
        image = operate(jnp.pad(direction, ((1, 1), (0, 0))), weights, centre, 1, MESH_NORTH_SOUTH)
        residual = residual - image
        recur_next = 1.0 / (2.0 * sigma - recur)
        direction = recur_next * recur * direction + 2.0 * recur_next / delta * residual
        recur = recur_next
    return (diffused_heat, solution + direction)
```

```python
import functools
import math

import jax
import jax.numpy as jnp
from jax import lax
from jax.experimental import pallas as pl
from jax.experimental.pallas import tpu as pltpu
from jax.sharding import Mesh
from jax.sharding import PartitionSpec as P

ITERS = 4
CHUNK = 6


def mix_kernel(
    spacing_ref, wet_ref, water_ref, heat_hbm, conduct_hbm, out_hbm, forcing_ref,
    heat_buf, conduct_buf, ratio_buf, value_buf, heat_sem, conduct_sem, out_sem,
):
    levels, rows, cols = heat_buf.shape
    chunks = levels // CHUNK

    def fetch(chunk):
        first = chunk * CHUNK
        count = min(CHUNK, levels - 1 - first)
        return (
            pltpu.make_async_copy(
                heat_hbm.at[pl.ds(first, CHUNK)], heat_buf.at[pl.ds(first, CHUNK)], heat_sem.at[chunk]
            ),
            pltpu.make_async_copy(
                conduct_hbm.at[pl.ds(first, count)], conduct_buf.at[pl.ds(first, count)], conduct_sem.at[chunk]
            ),
        )

    def flush(chunk):
        first = chunk * CHUNK
        return pltpu.make_async_copy(
            value_buf.at[pl.ds(first, CHUNK)], out_hbm.at[pl.ds(first, CHUNK)], out_sem.at[chunk]
        )

    for chunk in range(chunks):
        for copy in fetch(chunk):
            copy.start()
    wet = wet_ref[...]
    zero = jnp.zeros((rows, cols), jnp.float32)

    def down(level, carry, last=False):
        couple_prev, ratio_prev, value_prev = carry
        spacing = spacing_ref[level]
        if last:
            couple = zero
        else:
            couple = jnp.where(level + 1 < wet, conduct_buf[level].astype(jnp.float32), 0.0)
        source = spacing * heat_buf[level].astype(jnp.float32)
        pivot = spacing + couple_prev + couple - couple_prev * ratio_prev
        inverse = 1.0 / pivot
        ratio = couple * inverse
        value = (source + couple_prev * value_prev) * inverse
        ratio_buf[level] = ratio
        value_buf[level] = value
        return couple, ratio, value

    carry = (zero, zero, zero)
    for chunk in range(chunks):
        for copy in fetch(chunk):
            copy.wait()
        first = chunk * CHUNK
        stop = min(first + CHUNK, levels - 1)
        carry = lax.fori_loop(first, stop, down, carry)
    carry = down(levels - 1, carry, last=True)

    def up(step, carry, first):
        below, total = carry
        level = first + CHUNK - 1 - step
        result = value_buf[level] + ratio_buf[level] * below
        value_buf[level] = result
        total = total + jnp.where(level < wet, spacing_ref[level] * result, 0.0)
        return result, total

    carry = (zero, zero)
    for chunk in reversed(range(chunks)):
        carry = lax.fori_loop(0, CHUNK, functools.partial(up, first=chunk * CHUNK), carry)
        flush(chunk).start()
    forcing_ref[...] = water_ref[...].astype(jnp.float32) * carry[1] * (1.0 / math.sqrt(levels))
    for chunk in reversed(range(chunks)):
        flush(chunk).wait()


def mix(heat, conduct, spacing, wet, water):
    levels, rows, cols = heat.shape
    chunks = levels // CHUNK
    vmem = pl.BlockSpec(memory_space=pltpu.VMEM)
    hbm = pl.BlockSpec(memory_space=pl.ANY)
    return pl.pallas_call(
        mix_kernel,
        in_specs=[pl.BlockSpec(memory_space=pltpu.SMEM), vmem, vmem, hbm, hbm],
        out_specs=[hbm, vmem],
        out_shape=[
            jax.ShapeDtypeStruct((levels, rows, cols), jnp.float32),
            jax.ShapeDtypeStruct((rows, cols), jnp.float32),
        ],
        scratch_shapes=[
            pltpu.VMEM((levels, rows, cols), heat.dtype),
            pltpu.VMEM((levels, rows, cols), conduct.dtype),
            pltpu.VMEM((levels, rows, cols), jnp.float32),
            pltpu.VMEM((levels, rows, cols), jnp.float32),
            pltpu.SemaphoreType.DMA((chunks,)),
            pltpu.SemaphoreType.DMA((chunks,)),
            pltpu.SemaphoreType.DMA((chunks,)),
        ],
        name="mix",
    )(spacing, wet, water, heat, conduct)


ROW = ("row_0", "row_1")
COL = ("col_0", "col_1")
HALO = ITERS
VMEM = pl.BlockSpec(memory_space=pltpu.VMEM)
surface_term = 0.5


def rows_kernel(forcing_ref, depth_ref, water_ref, north_ref, south_ref):
    rows = forcing_ref.shape[0]
    for slot, field in enumerate((forcing_ref[...], depth_ref[...], water_ref[...].astype(jnp.float32))):
        north_ref[slot * HALO : (slot + 1) * HALO] = field[:HALO]
        south_ref[slot * HALO : (slot + 1) * HALO] = field[rows - HALO :]


def edge_kernel(forcing_ref, depth_ref, water_ref, north_ref, south_ref, tall_ref, edge_ref):
    rows, cols = forcing_ref.shape
    tall = rows + 2 * HALO
    lane = lax.broadcasted_iota(jnp.int32, (tall, 128), 1)
    for slot, field in enumerate((forcing_ref[...], depth_ref[...], water_ref[...].astype(jnp.float32))):
        tall_ref[slot, :rows] = field
        tall_ref[slot, rows : rows + HALO] = south_ref[slot * HALO : (slot + 1) * HALO]
        tall_ref[slot, rows + HALO :] = north_ref[slot * HALO : (slot + 1) * HALO]
        edge_ref[slot] = jnp.where(lane < 64, tall_ref[slot, :, :128], tall_ref[slot, :, cols - 128 :])


def around(field):
    tall, wide = field.shape
    beside = pltpu.roll(field, 1, 0) + pltpu.roll(field, tall - 1, 0)
    slant = field + 0.5 * beside
    return beside + (pltpu.roll(slant, 1, 1) + pltpu.roll(slant, wide - 1, 1))


def weights_kernel(tall_ref, west_ref, east_ref, wide_ref, centre_ref, bound_ref):
    tall, cols = tall_ref.shape[1:]
    rows = tall - 2 * HALO
    lane = lax.broadcasted_iota(jnp.int32, (tall, 128), 1)
    full = []
    for slot in range(3):
        side = jnp.where(lane < HALO, east_ref[slot], jnp.where(lane >= 128 - HALO, west_ref[slot], 0.0))
        full.append(jnp.concatenate([tall_ref[slot], side], axis=1))
    forcing, depth, ocean = full
    wet_depth = depth * ocean
    centre = surface_term + 0.5 * (wet_depth * around(ocean) + ocean * around(wet_depth))
    wide_ref[0] = forcing
    wide_ref[1] = wet_depth
    wide_ref[2] = ocean
    centre_ref[...] = centre
    own = 2.0 * centre[:rows, :cols] - surface_term
    high = jnp.max(jnp.max(own, axis=0, keepdims=True), axis=1, keepdims=True)
    bound_ref[...] = jnp.broadcast_to(high, bound_ref.shape)


def solve_kernel(bound_ref, wide_ref, centre_ref, height_ref):
    rows, cols = height_ref.shape
    tall, wide = centre_ref.shape
    top = jnp.max(bound_ref[...], axis=0, keepdims=True)
    top = jnp.concatenate([top] * (wide // 128), axis=1)
    theta = 0.5 * (top + surface_term)
    delta = 0.5 * (top - surface_term)
    sigma = theta / delta
    wet_depth, ocean, centre = wide_ref[1], wide_ref[2], centre_ref[...]
    residual = wide_ref[0]
    direction = residual / theta
    total = direction
    recur = 1.0 / sigma
    for step in range(ITERS):
        image = centre * direction - 0.5 * (
            wet_depth * around(ocean * direction) + ocean * around(wet_depth * direction)
        )
        residual = residual - image
        recur_next = 1.0 / (2.0 * sigma - recur)
        direction = (recur_next * recur) * direction + (2.0 * recur_next / delta) * residual
        recur = recur_next
        total = total + direction
    height_ref[...] = total[:rows, :cols]


def call(kernel, outs, *args):
    shapes = [jax.ShapeDtypeStruct(shape, jnp.float32) for shape in outs]
    return pl.pallas_call(
        kernel, in_specs=[VMEM] * len(args), out_specs=[VMEM] * len(outs), out_shape=shapes, name=kernel.__name__
    )(*args)


def local(heat, conduct, spacing, wet, water, depth):
    rows, cols = depth.shape
    tall, wide = rows + 2 * HALO, cols + 128
    devices = lax.axis_size(ROW) * lax.axis_size(COL)
    diffused, forcing = mix(heat, conduct, spacing, wet, water)
    to_north, to_south = call(rows_kernel, [(3 * HALO, cols)] * 2, forcing, depth, water)
    down = [(i, i + 1) for i in range(lax.axis_size(ROW) - 1)]
    north = lax.ppermute(to_south, ROW, down)
    south = lax.ppermute(to_north, ROW, [(b, a) for a, b in down])
    fields, edge = call(edge_kernel, [(3, tall, cols), (3, tall, 128)], forcing, depth, water, north, south)
    ring = [(i, (i + 1) % lax.axis_size(COL)) for i in range(lax.axis_size(COL))]
    west = lax.ppermute(edge, COL, ring)
    east = lax.ppermute(edge, COL, [(b, a) for a, b in ring])
    full, centre, bound = call(
        weights_kernel, [(3, tall, wide), (tall, wide), (devices, 128)], fields, west, east
    )
    bounds = lax.all_to_all(bound, ROW + COL, 0, 0, tiled=True)
    (height,) = call(solve_kernel, [(rows, cols)], bounds, full, centre)
    return diffused, height


def solution(mesh):
    torus = Mesh(mesh.devices.reshape(16, 4, 8, 2), ROW + COL)
    return jax.shard_map(
        local,
        mesh=torus,
        in_specs=(P(None, ROW, COL), P(None, ROW, COL), P(), P(ROW, COL), P(ROW, COL), P(ROW, COL)),
        out_specs=(P(None, ROW, COL), P(ROW, COL)),
        check_vma=False,
    )
```

```python
import functools
import math

import jax
import jax.numpy as jnp
from jax import lax
from jax.experimental import pallas as pl
from jax.experimental.pallas import tpu as pltpu
from jax.sharding import Mesh
from jax.sharding import PartitionSpec as P

ITERS = 4
CHUNK = 6
ROW = ("row_0", "row_1")
COL = ("col_0", "col_1")
HALO = ITERS
VMEM = pl.BlockSpec(memory_space=pltpu.VMEM)
SMEM = pl.BlockSpec(memory_space=pltpu.SMEM)
surface_term = 0.5


def mix_kernel(
    spacing_ref, wet_hbm, water_hbm, depth_hbm, heat_hbm, conduct_hbm,
    out_hbm, forcing_hbm, north_hbm, south_hbm,
    forcing_ref, north_ref, south_ref, wet_ref, water_ref, depth_ref, heat_buf, conduct_buf, ratio_buf, value_buf,
    plane_sem, edge_sem, heat_sem, conduct_sem, out_sem,
):
    levels, rows, cols = heat_buf.shape
    chunks = levels // CHUNK
    planes = [
        pltpu.make_async_copy(source, target, plane_sem.at[slot])
        for slot, (source, target) in enumerate(
            ((wet_hbm, wet_ref), (water_hbm, water_ref), (depth_hbm, depth_ref))
        )
    ]
    planes[0].start()

    def fetch(chunk):
        first = chunk * CHUNK
        count = min(CHUNK, levels - 1 - first)
        return (
            pltpu.make_async_copy(
                heat_hbm.at[pl.ds(first, CHUNK)], heat_buf.at[pl.ds(first, CHUNK)], heat_sem.at[chunk]
            ),
            pltpu.make_async_copy(
                conduct_hbm.at[pl.ds(first, count)], conduct_buf.at[pl.ds(first, count)], conduct_sem.at[chunk]
            ),
        )

    def flush(chunk):
        first = chunk * CHUNK
        return pltpu.make_async_copy(
            value_buf.at[pl.ds(first, CHUNK)], out_hbm.at[pl.ds(first, CHUNK)], out_sem.at[chunk]
        )

    for chunk in range(chunks):
        for copy in fetch(chunk):
            copy.start()
    planes[1].start()
    planes[2].start()
    planes[0].wait()
    wet = wet_ref[...]
    zero = jnp.zeros((rows, cols), jnp.float32)

    def down(level, carry, last=False):
        couple_prev, ratio_prev, value_prev = carry
        spacing = spacing_ref[level]
        if last:
            couple = zero
        else:
            couple = jnp.where(level + 1 < wet, conduct_buf[level].astype(jnp.float32), 0.0)
        source = spacing * heat_buf[level].astype(jnp.float32)
        pivot = spacing + couple_prev + couple - couple_prev * ratio_prev
        inverse = 1.0 / pivot
        ratio = couple * inverse
        value = (source + couple_prev * value_prev) * inverse
        ratio_buf[level] = ratio
        value_buf[level] = value
        return couple, ratio, value

    carry = (zero, zero, zero)
    for chunk in range(chunks):
        for copy in fetch(chunk):
            copy.wait()
        first = chunk * CHUNK
        stop = min(first + CHUNK, levels - 1)
        carry = lax.fori_loop(first, stop, down, carry)
    carry = down(levels - 1, carry, last=True)

    def up(step, carry, first):
        below, total = carry
        level = first + CHUNK - 1 - step
        result = value_buf[level] + ratio_buf[level] * below
        value_buf[level] = result
        total = total + jnp.where(level < wet, spacing_ref[level] * result, 0.0)
        return result, total

    carry = (zero, zero)
    for chunk in reversed(range(chunks)):
        carry = lax.fori_loop(0, CHUNK, functools.partial(up, first=chunk * CHUNK), carry)
        flush(chunk).start()
    planes[1].wait()
    planes[2].wait()
    ocean = water_ref[...].astype(jnp.float32)
    forcing = ocean * carry[1] * (1.0 / math.sqrt(levels))
    forcing_ref[...] = forcing
    for slot, field in enumerate((forcing, depth_ref[...], ocean)):
        north_ref[slot * HALO : (slot + 1) * HALO] = field[:HALO]
        south_ref[slot * HALO : (slot + 1) * HALO] = field[rows - HALO :]
    edges = [
        pltpu.make_async_copy(source, target, edge_sem.at[slot])
        for slot, (source, target) in enumerate(
            ((north_ref, north_hbm), (south_ref, south_hbm), (forcing_ref, forcing_hbm))
        )
    ]
    for copy in edges:
        copy.start()
    for chunk in reversed(range(chunks)):
        flush(chunk).wait()
    for copy in edges:
        copy.wait()


def mix(heat, conduct, spacing, wet, water, depth):
    levels, rows, cols = heat.shape
    chunks = levels // CHUNK
    hbm = pl.BlockSpec(memory_space=pltpu.HBM)
    return pl.pallas_call(
        mix_kernel,
        in_specs=[pl.BlockSpec(memory_space=pltpu.SMEM), hbm, hbm, hbm, hbm, hbm],
        out_specs=[hbm, hbm, hbm, hbm],
        out_shape=[
            jax.ShapeDtypeStruct((levels, rows, cols), jnp.float32),
            jax.ShapeDtypeStruct((rows, cols), jnp.float32),
            jax.ShapeDtypeStruct((3 * HALO, cols), jnp.float32),
            jax.ShapeDtypeStruct((3 * HALO, cols), jnp.float32),
        ],
        scratch_shapes=[
            pltpu.VMEM((rows, cols), jnp.float32),
            pltpu.VMEM((3 * HALO, cols), jnp.float32),
            pltpu.VMEM((3 * HALO, cols), jnp.float32),
            pltpu.VMEM((rows, cols), wet.dtype),
            pltpu.VMEM((rows, cols), water.dtype),
            pltpu.VMEM((rows, cols), depth.dtype),
            pltpu.VMEM((levels, rows, cols), heat.dtype),
            pltpu.VMEM((levels, rows, cols), conduct.dtype),
            pltpu.VMEM((levels, rows, cols), jnp.float32),
            pltpu.VMEM((levels, rows, cols), jnp.float32),
            pltpu.SemaphoreType.DMA((3,)),
            pltpu.SemaphoreType.DMA((3,)),
            pltpu.SemaphoreType.DMA((chunks,)),
            pltpu.SemaphoreType.DMA((chunks,)),
            pltpu.SemaphoreType.DMA((chunks,)),
        ],
        name="mix",
    )(spacing, wet, water, depth, heat, conduct)


def around(field):
    tall, wide = field.shape
    beside = pltpu.roll(field, 1, 0) + pltpu.roll(field, tall - 1, 0)
    slant = field + 0.5 * beside
    return beside + (pltpu.roll(slant, 1, 1) + pltpu.roll(slant, wide - 1, 1))


def centre_of(wet_depth, ocean):
    return surface_term + 0.5 * (wet_depth * around(ocean) + ocean * around(wet_depth))


def most(field):
    return jnp.max(jnp.max(field, axis=0, keepdims=True), axis=1, keepdims=True)


def edge_kernel(forcing_ref, depth_ref, water_ref, north_ref, south_ref, tall_ref, slots_ref, pack_ref):
    rows, cols = forcing_ref.shape
    tall = rows + 2 * HALO
    lane = lax.broadcasted_iota(jnp.int32, (tall, 128), 1)
    for slot, field in enumerate((forcing_ref[...], depth_ref[...], water_ref[...].astype(jnp.float32))):
        tall_ref[slot, :HALO] = north_ref[slot * HALO : (slot + 1) * HALO]
        tall_ref[slot, HALO : HALO + rows] = field
        tall_ref[slot, HALO + rows :] = south_ref[slot * HALO : (slot + 1) * HALO]
        pack_ref[slot * tall : (slot + 1) * tall] = jnp.where(
            lane < 64, tall_ref[slot, :, :128], tall_ref[slot, :, cols - 128 :]
        )
    ocean = tall_ref[2]
    centre = centre_of(tall_ref[1] * ocean, ocean)
    row = lax.broadcasted_iota(jnp.int32, (tall, cols), 0)
    col = lax.broadcasted_iota(jnp.int32, (tall, cols), 1)
    inner = (row >= HALO) & (row < HALO + rows) & (col >= 1) & (col < cols - 1)
    pack_ref[3 * tall :] = jnp.broadcast_to(most(jnp.where(inner, centre, 0.0)), (128 - 3 * tall, 128))
    turned = pack_ref[...].T
    which = lax.broadcasted_iota(jnp.int32, (8, 128), 0)
    tile = jnp.where(which < HALO, turned[:8], turned[120:])
    for slot in range(slots_ref.shape[0] // 8):
        slots_ref[slot * 8 : (slot + 1) * 8] = tile


def weights_kernel(index_ref, slots_ref, tall_ref, wide_ref, centre_ref, bound_ref, pack_ref):
    tall, cols = tall_ref.shape[1:]
    devices = slots_ref.shape[0] // 8
    index = index_ref[0]
    which = lax.broadcasted_iota(jnp.int32, (8, 128), 0)
    east = slots_ref[pl.ds(pl.multiple_of(lax.rem(index + 1, devices) * 8, 8), 8)]
    west = slots_ref[pl.ds(pl.multiple_of(lax.rem(index + devices - 1, devices) * 8, 8), 8)]
    pack_ref[...] = jnp.zeros((128, 128), jnp.float32)
    pack_ref[:8] = jnp.where(which < HALO, east, 0.0)
    pack_ref[120:] = jnp.where(which >= HALO, west, 0.0)
    turned = pack_ref[...].T
    forcing, depth, ocean = (
        jnp.concatenate([tall_ref[slot], turned[slot * tall : (slot + 1) * tall]], axis=1) for slot in range(3)
    )
    wet_depth = depth * ocean
    wide_ref[0] = forcing
    wide_ref[1] = wet_depth
    wide_ref[2] = ocean
    centre_ref[...] = centre_of(wet_depth, ocean)
    slots = slots_ref[...]
    joint = pltpu.roll(slots, HALO, 0)
    joint_ocean = pltpu.roll(joint, 128 - tall, 1)
    joint_centre = centre_of(joint * joint_ocean, joint_ocean)
    row = lax.broadcasted_iota(jnp.int32, joint.shape, 0) % 8
    lane = lax.broadcasted_iota(jnp.int32, joint.shape, 1)
    seam = ((row == HALO - 1) | (row == HALO)) & (lane >= tall + HALO) & (lane < 2 * tall - HALO)
    high = most(jnp.where(seam, joint_centre, jnp.where(lane >= 3 * tall, slots, 0.0)))
    bound_ref[...] = jnp.broadcast_to(high, bound_ref.shape)


def solve_kernel(bounds_ref, wide_ref, centre_ref, height_ref):
    rows, cols = height_ref.shape
    tall, wide = centre_ref.shape
    top = 2.0 * jnp.max(bounds_ref[...], axis=0, keepdims=True) - surface_term
    top = jnp.concatenate([top] * (wide // 128), axis=1)
    theta = 0.5 * (top + surface_term)
    delta = 0.5 * (top - surface_term)
    sigma = theta / delta
    wet_depth, ocean, centre = wide_ref[1], wide_ref[2], centre_ref[...]
    residual = wide_ref[0]
    direction = residual / theta
    total = direction
    recur = 1.0 / sigma
    for step in range(ITERS):
        image = centre * direction - 0.5 * (
            wet_depth * around(ocean * direction) + ocean * around(wet_depth * direction)
        )
        residual = residual - image
        recur_next = 1.0 / (2.0 * sigma - recur)
        direction = (recur_next * recur) * direction + (2.0 * recur_next / delta) * residual
        recur = recur_next
        total = total + direction
    height_ref[...] = total[HALO : HALO + rows, :cols]


def call(kernel, outs, *args, scratch=()):
    return pl.pallas_call(
        kernel,
        in_specs=[SMEM if arg.ndim == 1 else VMEM for arg in args],
        out_specs=[VMEM] * len(outs),
        out_shape=[jax.ShapeDtypeStruct(shape, jnp.float32) for shape in outs],
        scratch_shapes=[pltpu.VMEM(shape, jnp.float32) for shape in scratch],
        compiler_params=pltpu.CompilerParams(vmem_limit_bytes=4 * 2**20),
        name=kernel.__name__,
    )(*args)


def local(heat, conduct, spacing, wet, water, depth):
    rows, cols = depth.shape
    tall, wide = rows + 2 * HALO, cols + 128
    ring = lax.axis_size(COL)
    index = lax.axis_index(COL).astype(jnp.int32).reshape(1)
    diffused, forcing, to_north, to_south = mix(heat, conduct, spacing, wet, water, depth)
    down = [(i, i + 1) for i in range(lax.axis_size(ROW) - 1)]
    north = lax.ppermute(to_south, ROW, down)
    south = lax.ppermute(to_north, ROW, [(b, a) for a, b in down])
    fields, slots = call(
        edge_kernel, [(3, tall, cols), (ring * 8, 128)], forcing, depth, water, north, south, scratch=[(128, 128)]
    )
    slots = lax.all_to_all(slots, COL, 0, 0, tiled=True)
    full, centre, bound = call(
        weights_kernel,
        [(3, tall, wide), (tall, wide), (lax.axis_size(ROW), 128)],
        index, slots, fields, scratch=[(128, 128)],
    )
    bounds = lax.all_to_all(bound, ROW, 0, 0, tiled=True)
    (height,) = call(solve_kernel, [(rows, cols)], bounds, full, centre)
    return diffused, height


def solution(mesh):
    torus = Mesh(mesh.devices.reshape(16, 4, 8, 2), ROW + COL)
    return jax.shard_map(
        local,
        mesh=torus,
        in_specs=(P(None, ROW, COL), P(None, ROW, COL), P(), P(ROW, COL), P(ROW, COL), P(ROW, COL)),
        out_specs=(P(None, ROW, COL), P(ROW, COL)),
        check_vma=False,
    )
```

```python
import functools
import math

import jax
import jax.numpy as jnp
from jax import lax
from jax.experimental import pallas as pl
from jax.experimental.pallas import tpu as pltpu
from jax.sharding import Mesh
from jax.sharding import PartitionSpec as P


ITERS = 4
CHUNK = 6
ROW = ("row_0", "row_1")
COL = ("col_0", "col_1")
HALO = ITERS
VMEM = pl.BlockSpec(memory_space=pltpu.VMEM)
SMEM = pl.BlockSpec(memory_space=pltpu.SMEM)
surface_term = 0.5


def mix_kernel(
    spacing_ref, wet_hbm, water_hbm, heat_hbm, conduct_hbm,
    out_hbm, forcing_hbm, north_hbm, south_hbm,
    forcing_ref, north_ref, south_ref, wet_ref, water_ref, heat_buf, conduct_buf, ratio_buf, value_buf,
    plane_sem, edge_sem, heat_sem, conduct_sem, out_sem,
):
    levels, rows, cols = heat_buf.shape
    chunks = levels // CHUNK
    planes = [
        pltpu.make_async_copy(source, target, plane_sem.at[slot])
        for slot, (source, target) in enumerate(((wet_hbm, wet_ref), (water_hbm, water_ref)))
    ]
    planes[0].start()

    def fetch(chunk):
        first = chunk * CHUNK
        count = min(CHUNK, levels - 1 - first)
        return (
            pltpu.make_async_copy(
                heat_hbm.at[pl.ds(first, CHUNK)], heat_buf.at[pl.ds(first, CHUNK)], heat_sem.at[chunk]
            ),
            pltpu.make_async_copy(
                conduct_hbm.at[pl.ds(first, count)], conduct_buf.at[pl.ds(first, count)], conduct_sem.at[chunk]
            ),
        )

    def flush(chunk):
        first = chunk * CHUNK
        return pltpu.make_async_copy(
            value_buf.at[pl.ds(first, CHUNK)], out_hbm.at[pl.ds(first, CHUNK)], out_sem.at[chunk]
        )

    for chunk in range(chunks):
        for copy in fetch(chunk):
            copy.start()
    planes[1].start()
    planes[0].wait()
    wet = wet_ref[...]
    zero = jnp.zeros((rows, cols), jnp.float32)

    def down(level, carry, last=False):
        couple_prev, ratio_prev, value_prev = carry
        spacing = spacing_ref[level]
        if last:
            couple = zero
        else:
            couple = jnp.where(level + 1 < wet, conduct_buf[level].astype(jnp.float32), 0.0)
        source = spacing * heat_buf[level].astype(jnp.float32)
        pivot = spacing + couple_prev + couple - couple_prev * ratio_prev
        inverse = 1.0 / pivot
        ratio = couple * inverse
        value = (source + couple_prev * value_prev) * inverse
        ratio_buf[level] = ratio
        value_buf[level] = value
        return couple, ratio, value

    carry = (zero, zero, zero)
    for chunk in range(chunks):
        for copy in fetch(chunk):
            copy.wait()
        first = chunk * CHUNK
        stop = min(first + CHUNK, levels - 1)
        carry = lax.fori_loop(first, stop, down, carry)
    carry = down(levels - 1, carry, last=True)

    def up(step, carry, first):
        below, total = carry
        level = first + CHUNK - 1 - step
        result = value_buf[level] + ratio_buf[level] * below
        value_buf[level] = result
        total = total + jnp.where(level < wet, spacing_ref[level] * result, 0.0)
        return result, total

    carry = (zero, zero)
    for chunk in reversed(range(chunks)):
        carry = lax.fori_loop(0, CHUNK, functools.partial(up, first=chunk * CHUNK), carry)
        flush(chunk).start()
    planes[1].wait()
    forcing = water_ref[...].astype(jnp.float32) * carry[1] * (1.0 / math.sqrt(levels))
    forcing_ref[...] = forcing
    north_ref[...] = forcing[:HALO]
    south_ref[...] = forcing[rows - HALO :]
    edges = [
        pltpu.make_async_copy(source, target, edge_sem.at[slot])
        for slot, (source, target) in enumerate(
            ((north_ref, north_hbm), (south_ref, south_hbm), (forcing_ref, forcing_hbm))
        )
    ]
    for copy in edges:
        copy.start()
    for chunk in reversed(range(chunks)):
        flush(chunk).wait()
    for copy in edges:
        copy.wait()


def mix(heat, conduct, spacing, wet, water):
    levels, rows, cols = heat.shape
    chunks = levels // CHUNK
    hbm = pl.BlockSpec(memory_space=pltpu.HBM)
    return pl.pallas_call(
        mix_kernel,
        in_specs=[SMEM, hbm, hbm, hbm, hbm],
        out_specs=[hbm, hbm, hbm, hbm],
        out_shape=[
            jax.ShapeDtypeStruct((levels, rows, cols), jnp.float32),
            jax.ShapeDtypeStruct((rows, cols), jnp.float32),
            jax.ShapeDtypeStruct((HALO, cols), jnp.float32),
            jax.ShapeDtypeStruct((HALO, cols), jnp.float32),
        ],
        scratch_shapes=[
            pltpu.VMEM((rows, cols), jnp.float32),
            pltpu.VMEM((HALO, cols), jnp.float32),
            pltpu.VMEM((HALO, cols), jnp.float32),
            pltpu.VMEM((rows, cols), wet.dtype),
            pltpu.VMEM((rows, cols), water.dtype),
            pltpu.VMEM((levels, rows, cols), heat.dtype),
            pltpu.VMEM((levels, rows, cols), conduct.dtype),
            pltpu.VMEM((levels, rows, cols), jnp.float32),
            pltpu.VMEM((levels, rows, cols), jnp.float32),
            pltpu.SemaphoreType.DMA((2,)),
            pltpu.SemaphoreType.DMA((3,)),
            pltpu.SemaphoreType.DMA((chunks,)),
            pltpu.SemaphoreType.DMA((chunks,)),
            pltpu.SemaphoreType.DMA((chunks,)),
        ],
        name="mix",
    )(spacing, wet, water, heat, conduct)


def around(field):
    tall, wide = field.shape
    beside = pltpu.roll(field, 1, 0) + pltpu.roll(field, tall - 1, 0)
    slant = field + 0.5 * beside
    return beside + (pltpu.roll(slant, 1, 1) + pltpu.roll(slant, wide - 1, 1))


def centre_of(wet_depth, ocean):
    return surface_term + 0.5 * (wet_depth * around(ocean) + ocean * around(wet_depth))


def most(field):
    return jnp.max(jnp.max(field, axis=0, keepdims=True), axis=1, keepdims=True)


def rows_kernel(depth_ref, water_ref, north_ref, south_ref):
    rows = depth_ref.shape[0]
    for slot, field in enumerate((depth_ref[...], water_ref[...].astype(jnp.float32))):
        north_ref[slot * HALO : (slot + 1) * HALO] = field[:HALO]
        south_ref[slot * HALO : (slot + 1) * HALO] = field[rows - HALO :]


def edge_kernel(depth_ref, water_ref, north_ref, south_ref, tall_ref, slots_ref, pack_ref):
    rows, cols = depth_ref.shape
    tall = rows + 2 * HALO
    lane = lax.broadcasted_iota(jnp.int32, (tall, 128), 1)
    for slot, field in enumerate((depth_ref[...], water_ref[...].astype(jnp.float32))):
        tall_ref[slot, :HALO] = north_ref[slot * HALO : (slot + 1) * HALO]
        tall_ref[slot, HALO : HALO + rows] = field
        tall_ref[slot, HALO + rows :] = south_ref[slot * HALO : (slot + 1) * HALO]
        pack_ref[slot * tall : (slot + 1) * tall] = jnp.where(
            lane < 64, tall_ref[slot, :, :128], tall_ref[slot, :, cols - 128 :]
        )
    ocean = tall_ref[1]
    centre = centre_of(tall_ref[0] * ocean, ocean)
    row = lax.broadcasted_iota(jnp.int32, (tall, cols), 0)
    col = lax.broadcasted_iota(jnp.int32, (tall, cols), 1)
    inner = (row >= HALO) & (row < HALO + rows) & (col >= 1) & (col < cols - 1)
    pack_ref[2 * tall :] = jnp.broadcast_to(most(jnp.where(inner, centre, 0.0)), (128 - 2 * tall, 128))
    turned = pack_ref[...].T
    which = lax.broadcasted_iota(jnp.int32, (8, 128), 0)
    tile = jnp.where(which < HALO, turned[:8], turned[120:])
    for slot in range(slots_ref.shape[0] // 8):
        slots_ref[slot * 8 : (slot + 1) * 8] = tile


def forcing_kernel(forcing_ref, north_ref, south_ref, tall_ref, edge_ref):
    rows, cols = forcing_ref.shape
    tall_ref[:HALO] = north_ref[...]
    tall_ref[HALO : HALO + rows] = forcing_ref[...]
    tall_ref[HALO + rows :] = south_ref[...]
    lane = lax.broadcasted_iota(jnp.int32, edge_ref.shape, 1)
    edge_ref[...] = jnp.where(lane < 64, tall_ref[:, :128], tall_ref[:, cols - 128 :])


def weights_kernel(index_ref, slots_ref, tall_ref, wide_ref, bound_ref, pack_ref):
    tall, _ = tall_ref.shape[1:]
    devices = slots_ref.shape[0] // 8
    index = index_ref[0]
    which = lax.broadcasted_iota(jnp.int32, (8, 128), 0)
    east = slots_ref[pl.ds(pl.multiple_of(lax.rem(index + 1, devices) * 8, 8), 8)]
    west = slots_ref[pl.ds(pl.multiple_of(lax.rem(index + devices - 1, devices) * 8, 8), 8)]
    slots = slots_ref[...]
    joint = pltpu.roll(slots, HALO, 0)
    joint_ocean = pltpu.roll(joint, 128 - tall, 1)
    joint_centre = centre_of(joint * joint_ocean, joint_ocean)
    row = lax.broadcasted_iota(jnp.int32, joint.shape, 0) % 8
    lane = lax.broadcasted_iota(jnp.int32, joint.shape, 1)
    seam = ((row == HALO - 1) | (row == HALO)) & (lane >= HALO) & (lane < tall - HALO)
    high = most(jnp.where(seam, joint_centre, jnp.where(lane >= 2 * tall, slots, 0.0)))
    bound_ref[...] = jnp.broadcast_to(high, bound_ref.shape)
    pack_ref[...] = jnp.zeros((128, 128), jnp.float32)
    pack_ref[:8] = jnp.where(which < HALO, east, 0.0)
    pack_ref[120:] = jnp.where(which >= HALO, west, 0.0)
    turned = pack_ref[...].T
    depth, ocean = (
        jnp.concatenate([tall_ref[slot], turned[slot * tall : (slot + 1) * tall]], axis=1) for slot in range(2)
    )
    wet_depth = depth * ocean
    wide_ref[0] = wet_depth
    wide_ref[1] = ocean
    wide_ref[2] = centre_of(wet_depth, ocean)


def solve_kernel(bounds_ref, wide_ref, tall_ref, west_ref, east_ref, height_ref):
    rows, cols = height_ref.shape
    tall, wide = wide_ref.shape[1:]
    top = 2.0 * jnp.max(bounds_ref[...], axis=0, keepdims=True) - surface_term
    top = jnp.concatenate([top] * (wide // 128), axis=1)
    theta = 0.5 * (top + surface_term)
    delta = 0.5 * (top - surface_term)
    sigma = theta / delta
    wet_depth, ocean, centre = wide_ref[0], wide_ref[1], wide_ref[2]
    lane = lax.broadcasted_iota(jnp.int32, (tall, 128), 1)
    side = jnp.where(lane < HALO, east_ref[...], jnp.where(lane >= 128 - HALO, west_ref[...], 0.0))
    residual = jnp.concatenate([tall_ref[...], side], axis=1)
    direction = residual / theta
    total = direction
    recur = 1.0 / sigma
    for _ in range(ITERS):
        image = centre * direction - 0.5 * (
            wet_depth * around(ocean * direction) + ocean * around(wet_depth * direction)
        )
        residual = residual - image
        recur_next = 1.0 / (2.0 * sigma - recur)
        direction = (recur_next * recur) * direction + (2.0 * recur_next / delta) * residual
        recur = recur_next
        total = total + direction
    height_ref[...] = total[HALO : HALO + rows, :cols]


def call(kernel, outs, *args, scratch=(), limit=4 * 2**20):
    return pl.pallas_call(
        kernel,
        in_specs=[SMEM if arg.ndim == 1 else VMEM for arg in args],
        out_specs=[VMEM] * len(outs),
        out_shape=[jax.ShapeDtypeStruct(shape, jnp.float32) for shape in outs],
        scratch_shapes=[pltpu.VMEM(shape, jnp.float32) for shape in scratch],
        compiler_params=pltpu.CompilerParams(vmem_limit_bytes=limit),
    )(*args)


def step(heat, conduct, spacing, wet, water, depth):
    rows, cols = depth.shape
    tall, wide = rows + 2 * HALO, cols + 128
    ring = lax.axis_size(COL)
    index = lax.axis_index(COL).astype(jnp.int32).reshape(1)
    down = [(i, i + 1) for i in range(lax.axis_size(ROW) - 1)]
    right = [(i, (i + 1) % ring) for i in range(ring)]
    up, left = ([(b, a) for a, b in pairs] for pairs in (down, right))

    to_north, to_south = call(rows_kernel, [(2 * HALO, cols)] * 2, depth, water)
    north = lax.ppermute(to_south, ROW, down)
    south = lax.ppermute(to_north, ROW, up)
    diffused, forcing, forcing_north, forcing_south = mix(heat, conduct, spacing, wet, water)
    fields, slots = call(
        edge_kernel, [(2, tall, cols), (ring * 8, 128)], depth, water, north, south, scratch=[(128, 128)]
    )
    from_north = lax.ppermute(forcing_south, ROW, down)
    from_south = lax.ppermute(forcing_north, ROW, up)
    slots = lax.all_to_all(slots, COL, 0, 0, tiled=True)
    forcing, edge = call(forcing_kernel, [(tall, cols), (tall, 128)], forcing, from_north, from_south)
    full, bound = call(
        weights_kernel, [(3, tall, wide), (lax.axis_size(ROW), 128)], index, slots, fields, scratch=[(128, 128)]
    )
    west = lax.ppermute(edge, COL, right)
    east = lax.ppermute(edge, COL, left)
    bounds = lax.all_to_all(bound, ROW, 0, 0, tiled=True)
    (height,) = call(solve_kernel, [(rows, cols)], bounds, full, forcing, west, east)
    return diffused, height


def solution(mesh):
    torus = Mesh(mesh.devices.reshape(16, 4, 8, 2), ROW + COL)
    return jax.shard_map(
        step,
        mesh=torus,
        in_specs=(P(None, ROW, COL), P(None, ROW, COL), P(), P(ROW, COL), P(ROW, COL), P(ROW, COL)),
        out_specs=(P(None, ROW, COL), P(ROW, COL)),
        check_vma=False,
    )
```

```python
import functools
import math

import jax
import jax.numpy as jnp
from jax import lax
from jax.experimental import pallas as pl
from jax.experimental.pallas import tpu as pltpu
from jax.sharding import Mesh
from jax.sharding import PartitionSpec as P

ITERS = 4
CHUNK = 6
ROW = ("row_0", "row_1")
COL = ("col_0", "col_1")
HALO = ITERS
VMEM = pl.BlockSpec(memory_space=pltpu.VMEM)
SMEM = pl.BlockSpec(memory_space=pltpu.SMEM)
surface_term = 0.5


def mix_kernel(
    spacing_ref, wet_hbm, water_hbm, depth_hbm, heat_hbm, conduct_hbm,
    out_hbm, forcing_hbm, north_hbm, south_hbm,
    forcing_ref, north_ref, south_ref, wet_ref, water_ref, depth_ref, heat_buf, conduct_buf, ratio_buf, value_buf,
    plane_sem, edge_sem, heat_sem, conduct_sem, out_sem,
):
    levels, rows, cols = heat_buf.shape
    chunks = levels // CHUNK
    planes = [
        pltpu.make_async_copy(source, target, plane_sem.at[slot])
        for slot, (source, target) in enumerate(
            ((wet_hbm, wet_ref), (water_hbm, water_ref), (depth_hbm, depth_ref))
        )
    ]
    planes[0].start()

    def fetch(chunk):
        first = chunk * CHUNK
        count = min(CHUNK, levels - 1 - first)
        return (
            pltpu.make_async_copy(
                heat_hbm.at[pl.ds(first, CHUNK)], heat_buf.at[pl.ds(first, CHUNK)], heat_sem.at[chunk]
            ),
            pltpu.make_async_copy(
                conduct_hbm.at[pl.ds(first, count)], conduct_buf.at[pl.ds(first, count)], conduct_sem.at[chunk]
            ),
        )

    def flush(chunk):
        first = chunk * CHUNK
        return pltpu.make_async_copy(
            value_buf.at[pl.ds(first, CHUNK)], out_hbm.at[pl.ds(first, CHUNK)], out_sem.at[chunk]
        )

    for chunk in range(chunks):
        for copy in fetch(chunk):
            copy.start()
    planes[1].start()
    planes[2].start()
    planes[0].wait()
    wet = wet_ref[...]
    zero = jnp.zeros((rows, cols), jnp.float32)

    def down(level, carry, last=False):
        couple_prev, ratio_prev, value_prev = carry
        spacing = spacing_ref[level]
        if last:
            couple = zero
        else:
            couple = jnp.where(level + 1 < wet, conduct_buf[level].astype(jnp.float32), 0.0)
        source = spacing * heat_buf[level].astype(jnp.float32)
        pivot = spacing + couple_prev + couple - couple_prev * ratio_prev
        inverse = 1.0 / pivot
        ratio = couple * inverse
        value = (source + couple_prev * value_prev) * inverse
        ratio_buf[level] = ratio
        value_buf[level] = value
        return couple, ratio, value

    carry = (zero, zero, zero)
    for chunk in range(chunks):
        for copy in fetch(chunk):
            copy.wait()
        first = chunk * CHUNK
        stop = min(first + CHUNK, levels - 1)
        carry = lax.fori_loop(first, stop, down, carry)
    carry = down(levels - 1, carry, last=True)

    def up(step, carry, first):
        below, total = carry
        level = first + CHUNK - 1 - step
        result = value_buf[level] + ratio_buf[level] * below
        value_buf[level] = result
        total = total + jnp.where(level < wet, spacing_ref[level] * result, 0.0)
        return result, total

    carry = (zero, zero)
    for chunk in reversed(range(chunks)):
        carry = lax.fori_loop(0, CHUNK, functools.partial(up, first=chunk * CHUNK), carry)
        flush(chunk).start()
    planes[1].wait()
    planes[2].wait()
    ocean = water_ref[...].astype(jnp.float32)
    forcing = ocean * carry[1] * (1.0 / math.sqrt(levels))
    forcing_ref[...] = forcing
    for slot, field in enumerate((forcing, depth_ref[...], ocean)):
        north_ref[slot * HALO : (slot + 1) * HALO] = field[:HALO]
        south_ref[slot * HALO : (slot + 1) * HALO] = field[rows - HALO :]
    edges = [
        pltpu.make_async_copy(source, target, edge_sem.at[slot])
        for slot, (source, target) in enumerate(
            ((north_ref, north_hbm), (south_ref, south_hbm), (forcing_ref, forcing_hbm))
        )
    ]
    for copy in edges:
        copy.start()
    for chunk in reversed(range(chunks)):
        flush(chunk).wait()
    for copy in edges:
        copy.wait()


def mix(heat, conduct, spacing, wet, water, depth):
    levels, rows, cols = heat.shape
    chunks = levels // CHUNK
    hbm = pl.BlockSpec(memory_space=pltpu.HBM)
    return pl.pallas_call(
        mix_kernel,
        in_specs=[pl.BlockSpec(memory_space=pltpu.SMEM), hbm, hbm, hbm, hbm, hbm],
        out_specs=[hbm, hbm, hbm, hbm],
        out_shape=[
            jax.ShapeDtypeStruct((levels, rows, cols), jnp.float32),
            jax.ShapeDtypeStruct((rows, cols), jnp.float32),
            jax.ShapeDtypeStruct((3 * HALO, cols), jnp.float32),
            jax.ShapeDtypeStruct((3 * HALO, cols), jnp.float32),
        ],
        scratch_shapes=[
            pltpu.VMEM((rows, cols), jnp.float32),
            pltpu.VMEM((3 * HALO, cols), jnp.float32),
            pltpu.VMEM((3 * HALO, cols), jnp.float32),
            pltpu.VMEM((rows, cols), wet.dtype),
            pltpu.VMEM((rows, cols), water.dtype),
            pltpu.VMEM((rows, cols), depth.dtype),
            pltpu.VMEM((levels, rows, cols), heat.dtype),
            pltpu.VMEM((levels, rows, cols), conduct.dtype),
            pltpu.VMEM((levels, rows, cols), jnp.float32),
            pltpu.VMEM((levels, rows, cols), jnp.float32),
            pltpu.SemaphoreType.DMA((3,)),
            pltpu.SemaphoreType.DMA((3,)),
            pltpu.SemaphoreType.DMA((chunks,)),
            pltpu.SemaphoreType.DMA((chunks,)),
            pltpu.SemaphoreType.DMA((chunks,)),
        ],
        name="mix",
    )(spacing, wet, water, depth, heat, conduct)


def around(field):
    tall, wide = field.shape
    beside = pltpu.roll(field, 1, 0) + pltpu.roll(field, tall - 1, 0)
    slant = field + 0.5 * beside
    return beside + (pltpu.roll(slant, 1, 1) + pltpu.roll(slant, wide - 1, 1))


def centre_of(wet_depth, ocean):
    return surface_term + 0.5 * (wet_depth * around(ocean) + ocean * around(wet_depth))


def most(field):
    return jnp.max(jnp.max(field, axis=0, keepdims=True), axis=1, keepdims=True)


def edge_kernel(forcing_ref, depth_ref, water_ref, north_ref, south_ref, tall_ref, slots_ref, pack_ref):
    rows, cols = forcing_ref.shape
    tall = rows + 2 * HALO
    lane = lax.broadcasted_iota(jnp.int32, (tall, 128), 1)
    for slot, field in enumerate((forcing_ref[...], depth_ref[...], water_ref[...].astype(jnp.float32))):
        tall_ref[slot, :HALO] = north_ref[slot * HALO : (slot + 1) * HALO]
        tall_ref[slot, HALO : HALO + rows] = field
        tall_ref[slot, HALO + rows :] = south_ref[slot * HALO : (slot + 1) * HALO]
        pack_ref[slot * tall : (slot + 1) * tall] = jnp.where(
            lane < 64, tall_ref[slot, :, :128], tall_ref[slot, :, cols - 128 :]
        )
    ocean = tall_ref[2]
    centre = centre_of(tall_ref[1] * ocean, ocean)
    row = lax.broadcasted_iota(jnp.int32, (tall, cols), 0)
    col = lax.broadcasted_iota(jnp.int32, (tall, cols), 1)
    inner = (row >= HALO) & (row < HALO + rows) & (col >= 1) & (col < cols - 1)
    pack_ref[3 * tall :] = jnp.broadcast_to(most(jnp.where(inner, centre, 0.0)), (128 - 3 * tall, 128))
    turned = pack_ref[...].T
    which = lax.broadcasted_iota(jnp.int32, (8, 128), 0)
    tile = jnp.where(which < HALO, turned[:8], turned[120:])
    for slot in range(slots_ref.shape[0] // 8):
        slots_ref[slot * 8 : (slot + 1) * 8] = tile


def weights_kernel(order, index_ref, sent_ref, tall_ref, wide_ref, centre_ref, bound_ref, pack_ref, slots_ref):
    tall, cols = tall_ref.shape[1:]
    devices = len(order)
    for slot, device in enumerate(order):
        slots_ref[device * 8 : (device + 1) * 8] = sent_ref[slot * 8 : (slot + 1) * 8]
    index = index_ref[0]
    which = lax.broadcasted_iota(jnp.int32, (8, 128), 0)
    east = slots_ref[pl.ds(pl.multiple_of(lax.rem(index + 1, devices) * 8, 8), 8)]
    west = slots_ref[pl.ds(pl.multiple_of(lax.rem(index + devices - 1, devices) * 8, 8), 8)]
    pack_ref[...] = jnp.zeros((128, 128), jnp.float32)
    pack_ref[:8] = jnp.where(which < HALO, east, 0.0)
    pack_ref[120:] = jnp.where(which >= HALO, west, 0.0)
    turned = pack_ref[...].T
    forcing, depth, ocean = (
        jnp.concatenate([tall_ref[slot], turned[slot * tall : (slot + 1) * tall]], axis=1) for slot in range(3)
    )
    wet_depth = depth * ocean
    wide_ref[0] = forcing
    wide_ref[1] = wet_depth
    wide_ref[2] = ocean
    centre_ref[...] = centre_of(wet_depth, ocean)
    slots = slots_ref[...]
    joint = pltpu.roll(slots, HALO, 0)
    joint_ocean = pltpu.roll(joint, 128 - tall, 1)
    joint_centre = centre_of(joint * joint_ocean, joint_ocean)
    row = lax.broadcasted_iota(jnp.int32, joint.shape, 0) % 8
    lane = lax.broadcasted_iota(jnp.int32, joint.shape, 1)
    seam = ((row == HALO - 1) | (row == HALO)) & (lane >= tall + HALO) & (lane < 2 * tall - HALO)
    high = most(jnp.where(seam, joint_centre, jnp.where(lane >= 3 * tall, slots, 0.0)))
    bound_ref[...] = jnp.broadcast_to(high, bound_ref.shape)


def solve_kernel(bounds_ref, wide_ref, centre_ref, height_ref):
    rows, cols = height_ref.shape
    tall, wide = centre_ref.shape
    top = 2.0 * jnp.max(bounds_ref[...], axis=0, keepdims=True) - surface_term
    top = jnp.concatenate([top] * (wide // 128), axis=1)
    theta = 0.5 * (top + surface_term)
    delta = 0.5 * (top - surface_term)
    sigma = theta / delta
    wet_depth, ocean, centre = wide_ref[1], wide_ref[2], centre_ref[...]
    residual = wide_ref[0]
    direction = residual / theta
    total = direction
    recur = 1.0 / sigma
    for step in range(ITERS):
        image = centre * direction - 0.5 * (
            wet_depth * around(ocean * direction) + ocean * around(wet_depth * direction)
        )
        residual = residual - image
        recur_next = 1.0 / (2.0 * sigma - recur)
        direction = (recur_next * recur) * direction + (2.0 * recur_next / delta) * residual
        recur = recur_next
        total = total + direction
    height_ref[...] = total[HALO : HALO + rows, :cols]


def call(kernel, outs, *args, scratch=()):
    return pl.pallas_call(
        kernel,
        in_specs=[SMEM if arg.ndim == 1 else VMEM for arg in args],
        out_specs=[VMEM] * len(outs),
        out_shape=[jax.ShapeDtypeStruct(shape, jnp.float32) for shape in outs],
        scratch_shapes=[pltpu.VMEM(shape, jnp.float32) for shape in scratch],
        compiler_params=pltpu.CompilerParams(vmem_limit_bytes=4 * 2**20),
        name=getattr(kernel, "func", kernel).__name__,
    )(*args)


def far_first(axes):
    sizes = [lax.axis_size(axis) for axis in axes]

    def near(member):
        hops = 0
        for size in reversed(sizes):
            hops += min(member % size, size - member % size)
            member //= size
        return hops

    return sorted(range(math.prod(sizes)), key=lambda member: (-near(member), member))


def local(heat, conduct, spacing, wet, water, depth):
    rows, cols = depth.shape
    tall, wide = rows + 2 * HALO, cols + 128
    ring = lax.axis_size(COL)
    index = lax.axis_index(COL).astype(jnp.int32).reshape(1)
    order = far_first(COL)
    over_cols = [[row * ring + col for col in order] for row in range(lax.axis_size(ROW))]
    over_rows = [[row * ring + col for row in far_first(ROW)] for col in range(ring)]
    diffused, forcing, to_north, to_south = mix(heat, conduct, spacing, wet, water, depth)
    down = [(i, i + 1) for i in range(lax.axis_size(ROW) - 1)]
    north = lax.ppermute(to_south, ROW, down)
    south = lax.ppermute(to_north, ROW, [(b, a) for a, b in down])
    fields, slots = call(
        edge_kernel, [(3, tall, cols), (ring * 8, 128)], forcing, depth, water, north, south, scratch=[(128, 128)]
    )
    slots = lax.all_to_all(slots, ROW + COL, 0, 0, axis_index_groups=over_cols, tiled=True)
    full, centre, bound = call(
        functools.partial(weights_kernel, order),
        [(3, tall, wide), (tall, wide), (lax.axis_size(ROW), 128)],
        index, slots, fields, scratch=[(128, 128), (ring * 8, 128)],
    )
    bounds = lax.all_to_all(bound, ROW + COL, 0, 0, axis_index_groups=over_rows, tiled=True)
    (height,) = call(solve_kernel, [(rows, cols)], bounds, full, centre)
    return diffused, height


def solution(mesh):
    torus = Mesh(mesh.devices.reshape(16, 4, 8, 2), ROW + COL)
    return jax.shard_map(
        local,
        mesh=torus,
        in_specs=(P(None, ROW, COL), P(None, ROW, COL), P(), P(ROW, COL), P(ROW, COL), P(ROW, COL)),
        out_specs=(P(None, ROW, COL), P(ROW, COL)),
        check_vma=False,
    )
```

```python
import functools
import math

import jax
import jax.numpy as jnp
from jax import lax
from jax.experimental import pallas as pl
from jax.experimental.pallas import tpu as pltpu
from jax.sharding import Mesh
from jax.sharding import PartitionSpec as P


ITERS = 4
CHUNK = 6
ROW = ("row_0", "row_1")
COL = ("col_0", "col_1")
HALO = ITERS
VMEM = pl.BlockSpec(memory_space=pltpu.VMEM)
SMEM = pl.BlockSpec(memory_space=pltpu.SMEM)
surface_term = 0.5


def mix_kernel(
    starts, spacing_ref, wet_hbm, water_hbm, depth_hbm, heat_hbm, conduct_hbm, *refs,
):
    ends = depth_hbm is not None
    out_hbm, forcing_hbm, *refs = refs
    if ends:
        north_hbm, south_hbm, *refs = refs
    forcing_ref, wet_ref, water_ref, heat_buf, conduct_buf, ratio_buf, value_buf, *refs = refs
    plane_sem, forcing_sem, heat_sem, conduct_sem, out_sem, *refs = refs
    blocks, levels, block, _ = heat_buf.shape
    chunks = levels // CHUNK

    def plane(source, target, which):
        return [
            pltpu.make_async_copy(
                source.at[pl.ds(start, block)], target.at[pl.ds(slot * block, block)], plane_sem.at[which, slot]
            )
            for slot, start in enumerate(starts)
        ]

    def fetch(chunk):
        first = chunk * CHUNK
        count = min(CHUNK, levels - 1 - first)
        copies = []
        for slot, start in enumerate(starts):
            lines = pl.ds(start, block)
            copies.append(
                pltpu.make_async_copy(
                    heat_hbm.at[pl.ds(first, CHUNK), lines],
                    heat_buf.at[slot, pl.ds(first, CHUNK)],
                    heat_sem.at[slot, chunk],
                )
            )
            copies.append(
                pltpu.make_async_copy(
                    conduct_hbm.at[pl.ds(first, count), lines],
                    conduct_buf.at[slot, pl.ds(first, count)],
                    conduct_sem.at[slot, chunk],
                )
            )
        return copies

    def flush(chunk):
        first = chunk * CHUNK
        return [
            pltpu.make_async_copy(
                value_buf.at[pl.ds(first, CHUNK), pl.ds(slot * block, block)],
                out_hbm.at[pl.ds(first, CHUNK), pl.ds(start, block)],
                out_sem.at[slot, chunk],
            )
            for slot, start in enumerate(starts)
        ]

    wet_copies = plane(wet_hbm, wet_ref, 0)
    water_copies = plane(water_hbm, water_ref, 1)
    for copy in wet_copies:
        copy.start()
    for chunk in range(chunks):
        for copy in fetch(chunk):
            copy.start()
    for copy in water_copies:
        copy.start()
    if ends:
        depth_ref, north_ref, south_ref, edge_sem = refs
        depth_copies = plane(depth_hbm, depth_ref, 2)
        for copy in depth_copies:
            copy.start()
    for copy in wet_copies:
        copy.wait()
    wet = wet_ref[...]
    zero = jnp.zeros(wet.shape, jnp.float32)

    def joined(buf, level):
        return jnp.concatenate([buf[slot, level].astype(jnp.float32) for slot in range(blocks)], axis=0)

    def down(level, carry, last=False):
        couple_prev, ratio_prev, value_prev = carry
        spacing = spacing_ref[level]
        if last:
            couple = zero
        else:
            couple = jnp.where(level + 1 < wet, joined(conduct_buf, level), 0.0)
        source = spacing * joined(heat_buf, level)
        pivot = spacing + couple_prev + couple - couple_prev * ratio_prev
        inverse = 1.0 / pivot
        ratio = couple * inverse
        value = (source + couple_prev * value_prev) * inverse
        ratio_buf[level] = ratio
        value_buf[level] = value
        return couple, ratio, value

    carry = (zero, zero, zero)
    for chunk in range(chunks):
        for copy in fetch(chunk):
            copy.wait()
        first = chunk * CHUNK
        stop = min(first + CHUNK, levels - 1)
        carry = lax.fori_loop(first, stop, down, carry)
    carry = down(levels - 1, carry, last=True)

    def up(step, carry, first):
        below, total = carry
        level = first + CHUNK - 1 - step
        result = value_buf[level] + ratio_buf[level] * below
        value_buf[level] = result
        total = total + jnp.where(level < wet, spacing_ref[level] * result, 0.0)
        return result, total

    carry = (zero, zero)
    for chunk in reversed(range(chunks)):
        carry = lax.fori_loop(0, CHUNK, functools.partial(up, first=chunk * CHUNK), carry)
        for copy in flush(chunk):
            copy.start()
    for copy in water_copies:
        copy.wait()
    ocean = water_ref[...].astype(jnp.float32)
    forcing = ocean * carry[1] * (1.0 / math.sqrt(levels))
    forcing_ref[...] = forcing
    last = [pltpu.make_async_copy(forcing_ref, forcing_hbm, forcing_sem)]
    if ends:
        for copy in depth_copies:
            copy.wait()
        size = blocks * block
        for slot, field in enumerate((forcing, depth_ref[...], ocean)):
            north_ref[slot * HALO : (slot + 1) * HALO] = field[:HALO]
            south_ref[slot * HALO : (slot + 1) * HALO] = field[size - HALO :]
        last.append(pltpu.make_async_copy(north_ref, north_hbm, edge_sem.at[0]))
        last.append(pltpu.make_async_copy(south_ref, south_hbm, edge_sem.at[1]))
    for copy in last:
        copy.start()
    for chunk in reversed(range(chunks)):
        for copy in flush(chunk):
            copy.wait()
    for copy in last:
        copy.wait()


def first_kernel(starts, spacing, wet, water, depth, heat, conduct, *refs):
    mix_kernel(starts, spacing, wet, water, depth, heat, conduct, *refs)


def second_kernel(starts, spacing, wet, water, heat, conduct, begun, *refs):
    mix_kernel(starts, spacing, wet, water, None, heat, conduct, *refs)


def mix(starts, heat, conduct, spacing, wet, water, depth=None, begun=None):
    levels, rows, cols = heat.shape
    chunks, blocks, block = levels // CHUNK, len(starts), 8
    size = blocks * block
    hbm = pl.BlockSpec(memory_space=pltpu.HBM)
    shape = functools.partial(jax.ShapeDtypeStruct, dtype=jnp.float32)
    outs = [shape((levels, rows, cols)), shape((size, cols))]
    scratch = [
        pltpu.VMEM((size, cols), jnp.float32),
        pltpu.VMEM((size, cols), wet.dtype),
        pltpu.VMEM((size, cols), water.dtype),
        pltpu.VMEM((blocks, levels, block, cols), heat.dtype),
        pltpu.VMEM((blocks, levels, block, cols), conduct.dtype),
        pltpu.VMEM((levels, size, cols), jnp.float32),
        pltpu.VMEM((levels, size, cols), jnp.float32),
        pltpu.SemaphoreType.DMA((3, blocks)),
        pltpu.SemaphoreType.DMA,
        pltpu.SemaphoreType.DMA((blocks, chunks)),
        pltpu.SemaphoreType.DMA((blocks, chunks)),
        pltpu.SemaphoreType.DMA((blocks, chunks)),
    ]
    if begun is None:
        outs += [shape((3 * HALO, cols))] * 2
        scratch += [
            pltpu.VMEM((size, cols), depth.dtype),
            pltpu.VMEM((3 * HALO, cols), jnp.float32),
            pltpu.VMEM((3 * HALO, cols), jnp.float32),
            pltpu.SemaphoreType.DMA((2,)),
        ]
        kernel, args, aliases = first_kernel, (spacing, wet, water, depth, heat, conduct), {}
    else:
        kernel, args, aliases = second_kernel, (spacing, wet, water, heat, conduct, begun), {5: 0}
    return pl.pallas_call(
        functools.partial(kernel, starts),
        in_specs=[SMEM] + [hbm] * (len(args) - 1),
        out_specs=[hbm] * len(outs),
        out_shape=outs,
        scratch_shapes=scratch,
        input_output_aliases=aliases,
    )(*args)


def around(field):
    tall, wide = field.shape
    beside = pltpu.roll(field, 1, 0) + pltpu.roll(field, tall - 1, 0)
    slant = field + 0.5 * beside
    return beside + (pltpu.roll(slant, 1, 1) + pltpu.roll(slant, wide - 1, 1))


def centre_of(wet_depth, ocean):
    return surface_term + 0.5 * (wet_depth * around(ocean) + ocean * around(wet_depth))


def most(field):
    return jnp.max(jnp.max(field, axis=0, keepdims=True), axis=1, keepdims=True)


def edge_kernel(outer_ref, depth_ref, water_ref, north_ref, south_ref, tall_ref, slots_ref, pack_ref):
    rows, cols = depth_ref.shape
    tall = rows + 2 * HALO

    def outer(field):
        low = lax.broadcasted_iota(jnp.int32, (field.shape[0], 128), 1) < 64
        return jnp.where(low, field[:, :128], field[:, cols - 128 :])

    pack_ref[:HALO] = outer(north_ref[:HALO])
    pack_ref[HALO : HALO + rows] = outer_ref[...]
    pack_ref[HALO + rows : tall] = outer(south_ref[:HALO])
    for slot, field in enumerate((depth_ref[...], water_ref[...].astype(jnp.float32))):
        tall_ref[slot, :HALO] = north_ref[(slot + 1) * HALO : (slot + 2) * HALO]
        tall_ref[slot, HALO : HALO + rows] = field
        tall_ref[slot, HALO + rows :] = south_ref[(slot + 1) * HALO : (slot + 2) * HALO]
        pack_ref[(slot + 1) * tall : (slot + 2) * tall] = outer(tall_ref[slot])
    ocean = tall_ref[1]
    centre = centre_of(tall_ref[0] * ocean, ocean)
    row = lax.broadcasted_iota(jnp.int32, (tall, cols), 0)
    col = lax.broadcasted_iota(jnp.int32, (tall, cols), 1)
    inner = (row >= HALO) & (row < HALO + rows) & (col >= 1) & (col < cols - 1)
    pack_ref[3 * tall :] = jnp.broadcast_to(most(jnp.where(inner, centre, 0.0)), (128 - 3 * tall, 128))
    turned = pack_ref[...].T
    which = lax.broadcasted_iota(jnp.int32, (8, 128), 0)
    tile = jnp.where(which < HALO, turned[:8], turned[120:])
    for slot in range(slots_ref.shape[0] // 8):
        slots_ref[slot * 8 : (slot + 1) * 8] = tile


def weights_kernel(
    order, index_ref, sent_ref, forcing_ref, north_ref, south_ref, tall_ref,
    wide_ref, centre_ref, bound_ref, pack_ref, slots_ref, forced_ref,
):
    tall, _ = tall_ref.shape[1:]
    rows = tall - 2 * HALO
    forced_ref[:HALO] = north_ref[:HALO]
    forced_ref[HALO : HALO + rows] = forcing_ref[...]
    forced_ref[HALO + rows :] = south_ref[:HALO]
    devices = len(order)
    for slot, device in enumerate(order):
        slots_ref[device * 8 : (device + 1) * 8] = sent_ref[slot * 8 : (slot + 1) * 8]
    index = index_ref[0]
    which = lax.broadcasted_iota(jnp.int32, (8, 128), 0)
    east = slots_ref[pl.ds(pl.multiple_of(lax.rem(index + 1, devices) * 8, 8), 8)]
    west = slots_ref[pl.ds(pl.multiple_of(lax.rem(index + devices - 1, devices) * 8, 8), 8)]
    pack_ref[...] = jnp.zeros((128, 128), jnp.float32)
    pack_ref[:8] = jnp.where(which < HALO, east, 0.0)
    pack_ref[120:] = jnp.where(which >= HALO, west, 0.0)
    turned = pack_ref[...].T
    forcing, depth, ocean = (
        jnp.concatenate([field, turned[slot * tall : (slot + 1) * tall]], axis=1)
        for slot, field in enumerate((forced_ref[...], tall_ref[0], tall_ref[1]))
    )
    wet_depth = depth * ocean
    wide_ref[0] = forcing
    wide_ref[1] = wet_depth
    wide_ref[2] = ocean
    centre_ref[...] = centre_of(wet_depth, ocean)
    slots = slots_ref[...]
    joint = pltpu.roll(slots, HALO, 0)
    joint_ocean = pltpu.roll(joint, 128 - tall, 1)
    joint_centre = centre_of(joint * joint_ocean, joint_ocean)
    row = lax.broadcasted_iota(jnp.int32, joint.shape, 0) % 8
    lane = lax.broadcasted_iota(jnp.int32, joint.shape, 1)
    seam = ((row == HALO - 1) | (row == HALO)) & (lane >= tall + HALO) & (lane < 2 * tall - HALO)
    high = most(jnp.where(seam, joint_centre, jnp.where(lane >= 3 * tall, slots, 0.0)))
    bound_ref[...] = jnp.broadcast_to(high, bound_ref.shape)


def solve_kernel(bounds_ref, wide_ref, centre_ref, height_ref):
    rows, cols = height_ref.shape
    _, wide = centre_ref.shape
    top = 2.0 * jnp.max(bounds_ref[...], axis=0, keepdims=True) - surface_term
    top = jnp.concatenate([top] * (wide // 128), axis=1)
    theta = 0.5 * (top + surface_term)
    delta = 0.5 * (top - surface_term)
    sigma = theta / delta
    wet_depth, ocean, centre = wide_ref[1], wide_ref[2], centre_ref[...]
    residual = wide_ref[0]
    direction = residual / theta
    total = direction
    recur = 1.0 / sigma
    for _ in range(ITERS):
        image = centre * direction - 0.5 * (
            wet_depth * around(ocean * direction) + ocean * around(wet_depth * direction)
        )
        residual = residual - image
        recur_next = 1.0 / (2.0 * sigma - recur)
        direction = (recur_next * recur) * direction + (2.0 * recur_next / delta) * residual
        recur = recur_next
        total = total + direction
    height_ref[...] = total[HALO : HALO + rows, :cols]


def call(kernel, outs, *args, scratch=()):
    return pl.pallas_call(
        kernel,
        in_specs=[SMEM if arg.ndim == 1 else VMEM for arg in args],
        out_specs=[VMEM] * len(outs),
        out_shape=[jax.ShapeDtypeStruct(shape, jnp.float32) for shape in outs],
        scratch_shapes=[pltpu.VMEM(shape, jnp.float32) for shape in scratch],
        compiler_params=pltpu.CompilerParams(vmem_limit_bytes=4 * 2**20),
    )(*args)


def far_first(axes):
    sizes = [lax.axis_size(axis) for axis in axes]

    def near(member):
        hops = 0
        for size in reversed(sizes):
            hops += min(member % size, size - member % size)
            member //= size
        return hops

    return sorted(range(math.prod(sizes)), key=lambda member: (-near(member), member))


def step(heat, conduct, spacing, wet, water, depth):
    rows, cols = depth.shape
    tall, wide = rows + 2 * HALO, cols + 128
    ring = lax.axis_size(COL)
    index = lax.axis_index(COL).astype(jnp.int32).reshape(1)
    order = far_first(COL)
    over_cols = [[row * ring + col for col in order] for row in range(lax.axis_size(ROW))]
    over_rows = [[row * ring + col for row in far_first(ROW)] for col in range(ring)]
    blocks = list(range(0, rows, 8))
    outside, inside = [blocks[0], blocks[-1]], blocks[1:-1]
    diffused, forcing_ends, to_north, to_south = mix(outside, heat, conduct, spacing, wet, water, depth=depth)
    down = [(i, i + 1) for i in range(lax.axis_size(ROW) - 1)]
    north = lax.ppermute(to_south, ROW, down)
    south = lax.ppermute(to_north, ROW, [(b, a) for a, b in down])
    diffused, forcing_inside = mix(inside, heat, conduct, spacing, wet, water, begun=diffused)
    forcing = jnp.concatenate([forcing_ends[:8], forcing_inside, forcing_ends[8:]])
    low = lax.broadcasted_iota(jnp.int32, (rows, 128), 1) < 64
    outer = jnp.where(low, forcing[:, :128], forcing[:, cols - 128 :])
    fields, slots = call(
        edge_kernel, [(2, tall, cols), (ring * 8, 128)], outer, depth, water, north, south, scratch=[(128, 128)]
    )
    slots = lax.all_to_all(slots, ROW + COL, 0, 0, axis_index_groups=over_cols, tiled=True)
    full, centre, bound = call(
        functools.partial(weights_kernel, order),
        [(3, tall, wide), (tall, wide), (lax.axis_size(ROW), 128)],
        index, slots, forcing, north, south, fields, scratch=[(128, 128), (ring * 8, 128), (tall, cols)],
    )
    bounds = lax.all_to_all(bound, ROW + COL, 0, 0, axis_index_groups=over_rows, tiled=True)
    (height,) = call(solve_kernel, [(rows, cols)], bounds, full, centre)
    return diffused, height


def solution(mesh):
    torus = Mesh(mesh.devices.reshape(16, 4, 8, 2), ROW + COL)
    return jax.shard_map(
        step,
        mesh=torus,
        in_specs=(P(None, ROW, COL), P(None, ROW, COL), P(), P(ROW, COL), P(ROW, COL), P(ROW, COL)),
        out_specs=(P(None, ROW, COL), P(ROW, COL)),
        check_vma=False,
    )
```

```python
import functools
import math

import jax
import jax.numpy as jnp
from jax import lax
from jax.experimental import pallas as pl
from jax.experimental.pallas import tpu as pltpu
from jax.sharding import Mesh
from jax.sharding import PartitionSpec as P

ITERS = 4
CHUNK = 6
ROW = ("row_0", "row_1")
COL = ("col_0", "col_1")
HALO = ITERS
VMEM = pl.BlockSpec(memory_space=pltpu.VMEM)
SMEM = pl.BlockSpec(memory_space=pltpu.SMEM)
surface_term = 0.5


def mix_kernel(
    spacing_ref, wet_hbm, water_hbm, depth_hbm, heat_hbm, conduct_hbm,
    out_hbm, forcing_hbm, north_hbm, south_hbm,
    forcing_ref, north_ref, south_ref, wet_ref, water_ref, depth_ref, heat_buf, conduct_buf, ratio_buf, value_buf,
    plane_sem, edge_sem, heat_sem, conduct_sem, out_sem,
):
    levels, rows, cols = heat_buf.shape
    chunks = levels // CHUNK
    planes = [
        pltpu.make_async_copy(source, target, plane_sem.at[slot])
        for slot, (source, target) in enumerate(
            ((wet_hbm, wet_ref), (water_hbm, water_ref), (depth_hbm, depth_ref))
        )
    ]
    planes[0].start()

    def fetch(chunk):
        first = chunk * CHUNK
        count = min(CHUNK, levels - 1 - first)
        return (
            pltpu.make_async_copy(
                heat_hbm.at[pl.ds(first, CHUNK)], heat_buf.at[pl.ds(first, CHUNK)], heat_sem.at[chunk]
            ),
            pltpu.make_async_copy(
                conduct_hbm.at[pl.ds(first, count)], conduct_buf.at[pl.ds(first, count)], conduct_sem.at[chunk]
            ),
        )

    def flush(chunk):
        first = chunk * CHUNK
        return pltpu.make_async_copy(
            value_buf.at[pl.ds(first, CHUNK)], out_hbm.at[pl.ds(first, CHUNK)], out_sem.at[chunk]
        )

    for chunk in range(chunks):
        for copy in fetch(chunk):
            copy.start()
    planes[1].start()
    planes[2].start()
    planes[0].wait()
    wet = wet_ref[...]
    zero = jnp.zeros((rows, cols), jnp.float32)

    def down(level, carry, last=False):
        couple_prev, ratio_prev, value_prev = carry
        spacing = spacing_ref[level]
        if last:
            couple = zero
        else:
            couple = jnp.where(level + 1 < wet, conduct_buf[level].astype(jnp.float32), 0.0)
        source = spacing * heat_buf[level].astype(jnp.float32)
        pivot = spacing + couple_prev + couple - couple_prev * ratio_prev
        inverse = 1.0 / pivot
        ratio = couple * inverse
        value = (source + couple_prev * value_prev) * inverse
        ratio_buf[level] = ratio
        value_buf[level] = value
        return couple, ratio, value

    carry = (zero, zero, zero)
    for chunk in range(chunks):
        for copy in fetch(chunk):
            copy.wait()
        first = chunk * CHUNK
        stop = min(first + CHUNK, levels - 1)
        carry = lax.fori_loop(first, stop, down, carry)
    carry = down(levels - 1, carry, last=True)

    def up(step, carry, first):
        below, total = carry
        level = first + CHUNK - 1 - step
        result = value_buf[level] + ratio_buf[level] * below
        value_buf[level] = result
        total = total + jnp.where(level < wet, spacing_ref[level] * result, 0.0)
        return result, total

    carry = (zero, zero)
    for chunk in reversed(range(chunks)):
        carry = lax.fori_loop(0, CHUNK, functools.partial(up, first=chunk * CHUNK), carry)
        flush(chunk).start()
    planes[1].wait()
    planes[2].wait()
    ocean = water_ref[...].astype(jnp.float32)
    forcing = ocean * carry[1] * (1.0 / math.sqrt(levels))
    forcing_ref[...] = forcing
    for slot, field in enumerate((forcing, depth_ref[...], ocean)):
        north_ref[slot * HALO : (slot + 1) * HALO] = field[:HALO]
        south_ref[slot * HALO : (slot + 1) * HALO] = field[rows - HALO :]
    edges = [
        pltpu.make_async_copy(source, target, edge_sem.at[slot])
        for slot, (source, target) in enumerate(
            ((north_ref, north_hbm), (south_ref, south_hbm), (forcing_ref, forcing_hbm))
        )
    ]
    for copy in edges:
        copy.start()
    for chunk in reversed(range(chunks)):
        flush(chunk).wait()
    for copy in edges:
        copy.wait()


def mix(heat, conduct, spacing, wet, water, depth):
    levels, rows, cols = heat.shape
    chunks = levels // CHUNK
    hbm = pl.BlockSpec(memory_space=pltpu.HBM)
    return pl.pallas_call(
        mix_kernel,
        in_specs=[pl.BlockSpec(memory_space=pltpu.SMEM), hbm, hbm, hbm, hbm, hbm],
        out_specs=[hbm, hbm, hbm, hbm],
        out_shape=[
            jax.ShapeDtypeStruct((levels, rows, cols), jnp.float32),
            jax.ShapeDtypeStruct((rows, cols), jnp.float32),
            jax.ShapeDtypeStruct((3 * HALO, cols), jnp.float32),
            jax.ShapeDtypeStruct((3 * HALO, cols), jnp.float32),
        ],
        scratch_shapes=[
            pltpu.VMEM((rows, cols), jnp.float32),
            pltpu.VMEM((3 * HALO, cols), jnp.float32),
            pltpu.VMEM((3 * HALO, cols), jnp.float32),
            pltpu.VMEM((rows, cols), wet.dtype),
            pltpu.VMEM((rows, cols), water.dtype),
            pltpu.VMEM((rows, cols), depth.dtype),
            pltpu.VMEM((levels, rows, cols), heat.dtype),
            pltpu.VMEM((levels, rows, cols), conduct.dtype),
            pltpu.VMEM((levels, rows, cols), jnp.float32),
            pltpu.VMEM((levels, rows, cols), jnp.float32),
            pltpu.SemaphoreType.DMA((3,)),
            pltpu.SemaphoreType.DMA((3,)),
            pltpu.SemaphoreType.DMA((chunks,)),
            pltpu.SemaphoreType.DMA((chunks,)),
            pltpu.SemaphoreType.DMA((chunks,)),
        ],
        name="mix",
    )(spacing, wet, water, depth, heat, conduct)


def around(field):
    tall, wide = field.shape
    beside = pltpu.roll(field, 1, 0) + pltpu.roll(field, tall - 1, 0)
    slant = field + 0.5 * beside
    return beside + (pltpu.roll(slant, 1, 1) + pltpu.roll(slant, wide - 1, 1))


def centre_of(wet_depth, ocean):
    return surface_term + 0.5 * (wet_depth * around(ocean) + ocean * around(wet_depth))


def most(field):
    return jnp.max(jnp.max(field, axis=0, keepdims=True), axis=1, keepdims=True)


def edge_kernel(outer_ref, depth_ref, water_ref, north_ref, south_ref, tall_ref, slots_ref, pack_ref):
    rows, cols = depth_ref.shape
    tall = rows + 2 * HALO

    def outer(field):
        low = lax.broadcasted_iota(jnp.int32, (field.shape[0], 128), 1) < 64
        return jnp.where(low, field[:, :128], field[:, cols - 128 :])

    pack_ref[:HALO] = outer(north_ref[:HALO])
    pack_ref[HALO : HALO + rows] = outer_ref[...]
    pack_ref[HALO + rows : tall] = outer(south_ref[:HALO])
    for slot, field in enumerate((depth_ref[...], water_ref[...].astype(jnp.float32))):
        tall_ref[slot, :HALO] = north_ref[(slot + 1) * HALO : (slot + 2) * HALO]
        tall_ref[slot, HALO : HALO + rows] = field
        tall_ref[slot, HALO + rows :] = south_ref[(slot + 1) * HALO : (slot + 2) * HALO]
        pack_ref[(slot + 1) * tall : (slot + 2) * tall] = outer(tall_ref[slot])
    ocean = tall_ref[1]
    centre = centre_of(tall_ref[0] * ocean, ocean)
    row = lax.broadcasted_iota(jnp.int32, (tall, cols), 0)
    col = lax.broadcasted_iota(jnp.int32, (tall, cols), 1)
    inner = (row >= HALO) & (row < HALO + rows) & (col >= 1) & (col < cols - 1)
    pack_ref[3 * tall :] = jnp.broadcast_to(most(jnp.where(inner, centre, 0.0)), (128 - 3 * tall, 128))
    turned = pack_ref[...].T
    which = lax.broadcasted_iota(jnp.int32, (8, 128), 0)
    tile = jnp.where(which < HALO, turned[:8], turned[120:])
    for slot in range(slots_ref.shape[0] // 8):
        slots_ref[slot * 8 : (slot + 1) * 8] = tile


def weights_kernel(
    order, index_ref, sent_ref, forcing_ref, north_ref, south_ref, tall_ref,
    wide_ref, centre_ref, bound_ref, pack_ref, slots_ref, forced_ref,
):
    tall, cols = tall_ref.shape[1:]
    rows = tall - 2 * HALO
    forced_ref[:HALO] = north_ref[:HALO]
    forced_ref[HALO : HALO + rows] = forcing_ref[...]
    forced_ref[HALO + rows :] = south_ref[:HALO]
    devices = len(order)
    for slot, device in enumerate(order):
        slots_ref[device * 8 : (device + 1) * 8] = sent_ref[slot * 8 : (slot + 1) * 8]
    index = index_ref[0]
    which = lax.broadcasted_iota(jnp.int32, (8, 128), 0)
    east = slots_ref[pl.ds(pl.multiple_of(lax.rem(index + 1, devices) * 8, 8), 8)]
    west = slots_ref[pl.ds(pl.multiple_of(lax.rem(index + devices - 1, devices) * 8, 8), 8)]
    pack_ref[...] = jnp.zeros((128, 128), jnp.float32)
    pack_ref[:8] = jnp.where(which < HALO, east, 0.0)
    pack_ref[120:] = jnp.where(which >= HALO, west, 0.0)
    turned = pack_ref[...].T
    forcing, depth, ocean = (
        jnp.concatenate([field, turned[slot * tall : (slot + 1) * tall]], axis=1)
        for slot, field in enumerate((forced_ref[...], tall_ref[0], tall_ref[1]))
    )
    wet_depth = depth * ocean
    wide_ref[0] = forcing
    wide_ref[1] = wet_depth
    wide_ref[2] = ocean
    centre_ref[...] = centre_of(wet_depth, ocean)
    slots = slots_ref[...]
    joint = pltpu.roll(slots, HALO, 0)
    joint_ocean = pltpu.roll(joint, 128 - tall, 1)
    joint_centre = centre_of(joint * joint_ocean, joint_ocean)
    row = lax.broadcasted_iota(jnp.int32, joint.shape, 0) % 8
    lane = lax.broadcasted_iota(jnp.int32, joint.shape, 1)
    seam = ((row == HALO - 1) | (row == HALO)) & (lane >= tall + HALO) & (lane < 2 * tall - HALO)
    high = most(jnp.where(seam, joint_centre, jnp.where(lane >= 3 * tall, slots, 0.0)))
    bound_ref[...] = jnp.broadcast_to(high, bound_ref.shape)


def solve_kernel(bounds_ref, wide_ref, centre_ref, height_ref):
    rows, cols = height_ref.shape
    tall, wide = centre_ref.shape
    top = 2.0 * jnp.max(bounds_ref[...], axis=0, keepdims=True) - surface_term
    top = jnp.concatenate([top] * (wide // 128), axis=1)
    theta = 0.5 * (top + surface_term)
    delta = 0.5 * (top - surface_term)
    sigma = theta / delta
    wet_depth, ocean, centre = wide_ref[1], wide_ref[2], centre_ref[...]
    residual = wide_ref[0]
    direction = residual / theta
    total = direction
    recur = 1.0 / sigma
    for step in range(ITERS):
        image = centre * direction - 0.5 * (
            wet_depth * around(ocean * direction) + ocean * around(wet_depth * direction)
        )
        residual = residual - image
        recur_next = 1.0 / (2.0 * sigma - recur)
        direction = (recur_next * recur) * direction + (2.0 * recur_next / delta) * residual
        recur = recur_next
        total = total + direction
    height_ref[...] = total[HALO : HALO + rows, :cols]


def call(kernel, outs, *args, scratch=()):
    return pl.pallas_call(
        kernel,
        in_specs=[SMEM if arg.ndim == 1 else VMEM for arg in args],
        out_specs=[VMEM] * len(outs),
        out_shape=[jax.ShapeDtypeStruct(shape, jnp.float32) for shape in outs],
        scratch_shapes=[pltpu.VMEM(shape, jnp.float32) for shape in scratch],
        compiler_params=pltpu.CompilerParams(vmem_limit_bytes=4 * 2**20),
        name=getattr(kernel, "func", kernel).__name__,
    )(*args)


def far_first(axes):
    sizes = [lax.axis_size(axis) for axis in axes]

    def near(member):
        hops = 0
        for size in reversed(sizes):
            hops += min(member % size, size - member % size)
            member //= size
        return hops

    return sorted(range(math.prod(sizes)), key=lambda member: (-near(member), member))


def local(heat, conduct, spacing, wet, water, depth):
    rows, cols = depth.shape
    tall, wide = rows + 2 * HALO, cols + 128
    ring = lax.axis_size(COL)
    index = lax.axis_index(COL).astype(jnp.int32).reshape(1)
    order = far_first(COL)
    over_cols = [[row * ring + col for col in order] for row in range(lax.axis_size(ROW))]
    over_rows = [[row * ring + col for row in far_first(ROW)] for col in range(ring)]
    diffused, forcing, to_north, to_south = mix(heat, conduct, spacing, wet, water, depth)
    down = [(i, i + 1) for i in range(lax.axis_size(ROW) - 1)]
    north = lax.ppermute(to_south, ROW, down)
    south = lax.ppermute(to_north, ROW, [(b, a) for a, b in down])
    low = lax.broadcasted_iota(jnp.int32, (rows, 128), 1) < 64
    outer = jnp.where(low, forcing[:, :128], forcing[:, cols - 128 :])
    fields, slots = call(
        edge_kernel, [(2, tall, cols), (ring * 8, 128)], outer, depth, water, north, south, scratch=[(128, 128)]
    )
    slots = lax.all_to_all(slots, ROW + COL, 0, 0, axis_index_groups=over_cols, tiled=True)
    full, centre, bound = call(
        functools.partial(weights_kernel, order),
        [(3, tall, wide), (tall, wide), (lax.axis_size(ROW), 128)],
        index, slots, forcing, north, south, fields, scratch=[(128, 128), (ring * 8, 128), (tall, cols)],
    )
    bounds = lax.all_to_all(bound, ROW + COL, 0, 0, axis_index_groups=over_rows, tiled=True)
    (height,) = call(solve_kernel, [(rows, cols)], bounds, full, centre)
    return diffused, height


def solution(mesh):
    torus = Mesh(mesh.devices.reshape(16, 4, 8, 2), ROW + COL)
    return jax.shard_map(
        local,
        mesh=torus,
        in_specs=(P(None, ROW, COL), P(None, ROW, COL), P(), P(ROW, COL), P(ROW, COL), P(ROW, COL)),
        out_specs=(P(None, ROW, COL), P(ROW, COL)),
        check_vma=False,
    )
```
